16 devices in a mesh: dp: 2 (over z), ep: 8 (over y, x, core).
Axes of the slice: x: 2, y: 2, z: 2, core: 2. Of those that a mesh axis runs over, the one named last changes fastest.
Arguments:
- hidden: bfloat16 [65536, 768], P(('dp', 'ep')), parts along dimension 0
- logits: float32 [65536, 32], P(('dp', 'ep')), parts along dimension 0
- w_in: bfloat16 [32, 768, 3072], P('ep')
- w_out: bfloat16 [32, 3072, 768], P('ep')
- grad_out: bfloat16 [65536, 768], P(('dp', 'ep')), parts along dimension 0
Outputs:
- output 1: bfloat16 [65536, 768], P(('dp', 'ep')), parts along dimension 0
- output 2: bfloat16 [65536, 768], P(('dp', 'ep')), parts along dimension 0
- output 3: float32 [65536, 32], P(('dp', 'ep')), parts along dimension 0
- output 4: bfloat16 [64, 768, 3072], P(('dp', 'ep')), parts along dimension 0
- output 5: bfloat16 [64, 3072, 768], P(('dp', 'ep')), parts along dimension 0
There are 2 independent parts. The reference program is written for one: setup_inputs(seed, part) draws one part's arguments, and reference() takes and returns one part's arrays. A program takes and returns all parts, laid end to end along the dimension named above; an argument that names none is the same for every part.
All inputs are finite; a program needn't handle non-finite values.
Results may differ from the reference program's by a relative error of at most 0.00500352.
Values are sent between devices in bfloat16 or wider.
A program may use at most 1 GiB of HBM per device.

```python
import math
import jax
import jax.numpy as jnp
from jax import lax

TOK_DEV = 4096
GROUP = 8
EXPERTS = 32
D_MODEL = 768
D_FF = 3072
CAP_FACTOR = 2

TOKENS = TOK_DEV * GROUP
CAPACITY = TOKENS * CAP_FACTOR // EXPERTS
PAIR_CAP = 2 * CAPACITY // GROUP
LOGIT_STEP = 2.0 ** (1 - math.ceil(math.log2(TOKENS)))


def draw_logits(key):
    key_order, key_split, key_local, key_col, key_base = jax.random.split(key, 5)
    dev_order = jax.vmap(lambda one_key: jax.random.permutation(one_key, GROUP))(jax.random.split(key_order, EXPERTS))
    low_share = jax.random.randint(key_split, (EXPERTS, GROUP // 2), 0, PAIR_CAP + 1)
    low_share = jnp.where(jnp.arange(GROUP // 2)[None, :] == 0, 0, low_share)
    ordered = jnp.stack([low_share, PAIR_CAP - low_share], axis=-1).reshape(EXPERTS, GROUP)
    dev_counts = jnp.take_along_axis(ordered, jnp.argsort(dev_order, axis=1), axis=1)
    local_rank = jax.vmap(lambda one_key: jax.random.permutation(one_key, TOK_DEV))(jax.random.split(key_local, GROUP * EXPERTS))
    local_rank = local_rank.reshape(GROUP, EXPERTS, TOK_DEV)
    top_mask = local_rank < dev_counts.T[:, :, None]
    top_mask = jnp.transpose(top_mask, (0, 2, 1)).reshape(TOKENS, EXPERTS)
    col_rank = jax.vmap(lambda one_key: jax.random.permutation(one_key, TOKENS))(jax.random.split(key_col, EXPERTS)).T
    col_base = jax.random.randint(key_base, (EXPERTS,), 0, 3) * TOKENS
    score_int = col_rank + 3 * TOKENS * top_mask.astype(jnp.int32) + col_base[None, :]
    return score_int.astype(jnp.float32) * LOGIT_STEP


def setup_inputs(seed: int = 0, part: int = 0) -> dict:
    part_key = jax.random.fold_in(jax.random.key(seed), part)
    key_x, key_l, key_d = jax.random.split(part_key, 3)
    key_w1, key_w2 = jax.random.split(jax.random.key(seed + 1), 2)
    hidden = jax.random.normal(key_x, (TOKENS, D_MODEL), jnp.float32).astype(jnp.bfloat16)
    logits = draw_logits(key_l)
    w_in = (jax.random.normal(key_w1, (EXPERTS, D_MODEL, D_FF), jnp.float32) * D_MODEL ** -0.5).astype(jnp.bfloat16)
    w_out = (jax.random.normal(key_w2, (EXPERTS, D_FF, D_MODEL), jnp.float32) * D_FF ** -0.5).astype(jnp.bfloat16)
    grad_out = jax.random.normal(key_d, (TOKENS, D_MODEL), jnp.float32).astype(jnp.bfloat16)
    return {'hidden': hidden, 'logits': logits, 'w_in': w_in, 'w_out': w_out, 'grad_out': grad_out}


def reference(hidden, logits, w_in, w_out, grad_out):
    gates = jax.nn.softmax(logits, axis=-1)
    chosen_idx = lax.top_k(logits.T, CAPACITY)[1]
    gate_sel = jnp.take_along_axis(gates.T, chosen_idx, axis=1)

    def expert_step(carry, per_expert):
        mixed, dx_sum = carry
        idx_row, gate_row, w_one, w_two = per_expert
        rows_x = hidden[idx_row]
        rows_dout = grad_out[idx_row]
        pre_act = jnp.dot(rows_x, w_one, preferred_element_type=jnp.float32)
        act_val, gelu_back = jax.vjp(jax.nn.gelu, pre_act)
        hidden_act = act_val.astype(jnp.bfloat16)
        z_rows = jnp.dot(hidden_act, w_two, preferred_element_type=jnp.float32).astype(jnp.bfloat16)
        z_wide = z_rows.astype(jnp.float32)
        dout_wide = rows_dout.astype(jnp.float32)
        dgate_row = jnp.sum(dout_wide * z_wide, axis=-1)
        dz_rows = (gate_row[:, None] * dout_wide).astype(jnp.bfloat16)
        grad_two = jnp.dot(hidden_act.T, dz_rows, preferred_element_type=jnp.float32).astype(jnp.bfloat16)
        grad_act = jnp.dot(dz_rows, w_two.T, preferred_element_type=jnp.float32)
        grad_pre = gelu_back(grad_act)[0].astype(jnp.bfloat16)
        grad_one = jnp.dot(rows_x.T, grad_pre, preferred_element_type=jnp.float32).astype(jnp.bfloat16)
        dx_rows = jnp.dot(grad_pre, w_one.T, preferred_element_type=jnp.float32).astype(jnp.bfloat16)
        mixed = mixed.at[idx_row].add(gate_row[:, None] * z_wide)
        dx_sum = dx_sum.at[idx_row].add(dx_rows.astype(jnp.float32))
        return (mixed, dx_sum), (dgate_row, grad_one, grad_two)

    zero_rows = jnp.zeros((TOKENS, D_MODEL), jnp.float32)
    (mixed, dx_sum), (dgate_sel, grad_one, grad_two) = lax.scan(expert_step, (zero_rows, zero_rows), (chosen_idx, gate_sel, w_in, w_out))
    layer_out = (hidden.astype(jnp.float32) + mixed).astype(jnp.bfloat16)
    grad_hidden = (grad_out.astype(jnp.float32) + dx_sum).astype(jnp.bfloat16)
    dgate = jnp.zeros((EXPERTS, TOKENS), jnp.float32).at[jnp.arange(EXPERTS)[:, None], chosen_idx].set(dgate_sel).T
    grad_logits = gates * (dgate - jnp.sum(gates * dgate, axis=-1, keepdims=True))
    return (layer_out, grad_hidden, grad_logits, grad_one, grad_two)
```

```python
import functools

import jax
import jax.numpy as jnp
from jax import lax
from jax.experimental import pallas as pl
from jax.experimental.pallas import tpu as pltpu
from jax.sharding import PartitionSpec as P


CAP_FACTOR = 2
ALIGN = 16
F32 = jnp.float32
BF16 = jnp.bfloat16
SMEM = pltpu.SMEM
VMEM = pltpu.VMEM


def gate_kernel(pos_ref, len_ref, top_ref, den_ref, top_out, den_out):
    def row(e, _):
        def step(i, _):
            for u in range(ALIGN):
                k = i * ALIGN + u
                t = pos_ref[e, k]
                top_out[e, k] = top_ref[0, t]
                den_out[e, k] = den_ref[0, t]
            return 0

        return lax.fori_loop(0, len_ref[e] // ALIGN, step, 0)

    lax.fori_loop(0, pos_ref.shape[0], row, 0)


def candidate_stats(pos, length, top, den):
    shape = jax.ShapeDtypeStruct(pos.shape, F32)
    spec = pl.BlockSpec(memory_space=SMEM)
    return pl.pallas_call(
        gate_kernel,
        out_shape=(shape, shape),
        in_specs=[spec] * 4,
        out_specs=(spec, spec),
        cost_estimate=pl.CostEstimate(flops=30_000_000_000, bytes_accessed=400_000, transcendentals=0),
        name="candidate_stats",
    )(pos, length, top[None], den[None])


def compact_kernel(val_ref, len_ref, base_ref, fill_ref, out_ref):
    experts, sources, _ = val_ref.shape
    rows = out_ref.shape[1]
    for e in range(experts):
        for s in range(sources):
            base = base_ref[e, s]

            def step(i, _):
                for u in range(ALIGN):
                    k = i * ALIGN + u
                    out_ref[e, base + k] = val_ref[e, s, k]
                return 0

            lax.fori_loop(0, len_ref[e, s] // ALIGN, step, 0)
        total = base_ref[e, sources - 1] + len_ref[e, sources - 1]
        fill = fill_ref[e]

        def tail(i, _):
            for u in range(ALIGN):
                out_ref[e, total + i * ALIGN + u] = fill
            return 0

        lax.fori_loop(0, (rows - total) // ALIGN, tail, 0)


def compact(val, length, base, fill, rows):
    spec = pl.BlockSpec(memory_space=SMEM)
    return pl.pallas_call(
        compact_kernel,
        out_shape=jax.ShapeDtypeStruct((val.shape[0], rows), val.dtype),
        in_specs=[spec] * 4,
        out_specs=spec,
        cost_estimate=pl.CostEstimate(flops=15_000_000_000, bytes_accessed=200_000, transcendentals=0),
        name="compact",
    )(val, length, base, fill)


def spread_kernel(base_ref, len_ref, src_ref, *dst_refs):
    for p, dst_ref in enumerate(dst_refs):
        base = base_ref[p]

        def step(i, _):
            at = pl.multiple_of(i * ALIGN, ALIGN)
            frm = pl.multiple_of(base + at, ALIGN)
            dst_ref[pl.ds(at, ALIGN), :] = src_ref[pl.ds(frm, ALIGN), :]
            return 0

        lax.fori_loop(0, len_ref[p] // ALIGN, step, 0)


def spread(src, base, length, pair_cap):
    _, width = src.shape
    smem = pl.BlockSpec(memory_space=SMEM)
    vmem = pl.BlockSpec(memory_space=VMEM)
    sources = base.shape[0]
    return pl.pallas_call(
        spread_kernel,
        out_shape=[jax.ShapeDtypeStruct((pair_cap, width), src.dtype)] * sources,
        in_specs=[smem, smem, vmem],
        out_specs=[vmem] * sources,
        cost_estimate=pl.CostEstimate(flops=3_000_000_000, bytes_accessed=10_000_000, transcendentals=0),
        name="spread",
    )(base, length, src)


def spread_all_kernel(base_ref, len_ref, *refs):
    *src_refs, dst_ref = refs
    s = pl.program_id(0)
    for j, src_ref in enumerate(src_refs):
        base = base_ref[j, s]

        def step(i, _):
            at = pl.multiple_of(i * ALIGN, ALIGN)
            frm = pl.multiple_of(base + at, ALIGN)
            dst_ref[0, j, pl.ds(at, ALIGN), :] = src_ref[pl.ds(frm, ALIGN), :]
            return 0

        lax.fori_loop(0, len_ref[j, s] // ALIGN, step, 0)


def spread_all(srcs, base, length, pair_cap):
    rows, width = srcs[0].shape
    experts, sources = base.shape
    return pl.pallas_call(
        spread_all_kernel,
        out_shape=jax.ShapeDtypeStruct((sources, experts, pair_cap, width), srcs[0].dtype),
        grid_spec=pltpu.PrefetchScalarGridSpec(
            num_scalar_prefetch=2,
            grid=(sources,),
            in_specs=[pl.BlockSpec((rows, width), lambda s, *_: (0, 0), pipeline_mode=pl.Buffered(1))] * experts,
            out_specs=pl.BlockSpec((1, experts, pair_cap, width), lambda s, *_: (s, 0, 0, 0)),
        ),
        cost_estimate=pl.CostEstimate(flops=10_000_000_000, bytes_accessed=40_000_000, transcendentals=0),
        name="spread_all",
    )(base, length, *srcs)


def combine_kernel(views, scaled, marked, len_ref, pos_ref, start_ref, *refs):
    count = len(views)
    arrays = 1 + max(a for a, _ in views)
    rows_refs = [refs[a] if at is None else refs[a].at[at] for a, at in views]
    refs = refs[arrays:]
    if scaled:
        gate_ref, *refs = refs
    if marked:
        ids_ref, off_ref, val_ref, out_ref, dg_ref, acc, wide, held, sem = refs
        lane = lax.broadcasted_iota(jnp.int32, (1, dg_ref.shape[1]), 1)
        dg_ref[...] = jnp.zeros_like(dg_ref)
    else:
        out_ref, acc, wide, held, sem = refs
    tokens = acc.shape[0]
    block = 256
    slots = held.shape[0]
    copies = [pltpu.make_async_copy(r, held.at[q % slots], sem.at[q % slots]) for q, r in enumerate(rows_refs)]
    for q in range(min(slots - 1, count)):
        copies[q].start()

    def init(i, _):
        here = pl.ds(pl.multiple_of(i * block, block), block)
        acc[here, :] = start_ref[here, :].astype(F32)
        return 0

    lax.fori_loop(0, tokens // block, init, 0)
    for q in range(count):
        copies[q].wait()
        if q + slots - 1 < count:
            copies[q + slots - 1].start()
        rows_ref = held.at[q % slots]
        if marked:
            mark, off = lane == ids_ref[q], off_ref[q]

        def step(i, _):
            begin = pl.multiple_of(i * ALIGN, ALIGN)
            wide[...] = rows_ref[pl.ds(begin, ALIGN), :].astype(F32)
            for half in range(0, ALIGN, 8):
                toks, new, newd = [], [], []
                for u in range(half, half + 8):
                    t = pos_ref[q, begin + u]
                    row = wide[u : u + 1, :]
                    if scaled:
                        row = row * gate_ref[q, begin + u]
                    toks.append(t)
                    new.append(acc[pl.ds(t, 1), :] + row)
                    if marked:
                        newd.append(jnp.where(mark, val_ref[off + begin + u], dg_ref[pl.ds(t, 1), :]))
                for i_u, t in enumerate(toks):
                    acc[pl.ds(t, 1), :] = new[i_u]
                    if marked:
                        dg_ref[pl.ds(t, 1), :] = newd[i_u]
            return 0

        lax.fori_loop(0, len_ref[q] // ALIGN, step, 0)

    for q in range(count, len_ref.shape[0] if marked else 0):
        mark, off = lane == ids_ref[q], off_ref[q]

        def place(i, _):
            begin = i * ALIGN
            toks = [pos_ref[q, begin + u] for u in range(ALIGN)]
            new = [jnp.where(mark, val_ref[off + begin + u], dg_ref[pl.ds(t, 1), :]) for u, t in enumerate(toks)]
            for t, v in zip(toks, new):
                dg_ref[pl.ds(t, 1), :] = v
            return 0

        lax.fori_loop(0, len_ref[q] // ALIGN, place, 0)

    def final(i, _):
        here = pl.ds(pl.multiple_of(i * block, block), block)
        out_ref[here, :] = acc[here, :].astype(out_ref.dtype)
        return 0

    lax.fori_loop(0, tokens // block, final, 0)


def combine(start, rows, length, pos, out_dtype, gate=None, marks=None):
    pair_cap, width = rows[0].shape[-2:]
    if rows[0].ndim > 2:
        views = [(0, (d, j)) for d in range(rows[0].shape[0]) for j in range(rows[0].shape[1])]
    else:
        views = [(a, None) for a in range(len(rows))]
    tokens = start.shape[0]
    smem = pl.BlockSpec(memory_space=SMEM)
    vmem = pl.BlockSpec(memory_space=VMEM)
    in_specs = [smem] * 2 + [vmem] + [pl.BlockSpec(memory_space=pl.ANY)] * len(rows)
    args = [length, pos, start, *rows]
    if gate is not None:
        in_specs.append(smem)
        args.append(gate)
    out_shape = [jax.ShapeDtypeStruct((tokens, width), out_dtype)]
    if marks is not None:
        in_specs += [smem] * 3
        args += marks
        out_shape.append(jax.ShapeDtypeStruct((tokens, 128), F32))
    return pl.pallas_call(
        functools.partial(combine_kernel, views, gate is not None, marks is not None),
        out_shape=out_shape,
        in_specs=in_specs,
        out_specs=[vmem] * len(out_shape),
        scratch_shapes=[VMEM((tokens, width), F32), VMEM((ALIGN, width), F32), VMEM((4, pair_cap, width), BF16), pltpu.SemaphoreType.DMA((4,))],
        compiler_params=pltpu.CompilerParams(vmem_limit_bytes=60 * 1024 * 1024),
        cost_estimate=pl.CostEstimate(flops=1_500_000_000 * len(views), bytes_accessed=25_000_000, transcendentals=0),
        name="combine",
    )(*args)


GELU_A = (2.0 / 3.141592653589793) ** 0.5
GELU_B = 0.044715 * GELU_A


def dot_nn(a, b):
    return lax.dot_general(a, b, (((1,), (0,)), ((), ())), preferred_element_type=F32)


def dot_nt(a, b):
    return lax.dot_general(a, b, (((1,), (1,)), ((), ())), preferred_element_type=F32)


def forward_kernel(chunk, x_ref, w1_ref, w2_ref, z_ref, acc):
    @pl.when(pl.program_id(0) == 0)
    def _():
        acc[...] = jnp.zeros_like(acc)

    spans = [pl.ds(m, chunk) for m in range(0, x_ref.shape[0], chunk)]
    ahead = dot_nn(x_ref[spans[0], :], w1_ref[0])
    for i, here in enumerate(spans):
        a = ahead
        if i + 1 < len(spans):
            ahead = dot_nn(x_ref[spans[i + 1], :], w1_ref[0])
        t = jnp.tanh(a * (GELU_A + GELU_B * (a * a)))
        h = (a * (0.5 + 0.5 * t)).astype(BF16)
        acc[here, :] += dot_nn(h, w2_ref[0])

    @pl.when(pl.program_id(0) == pl.num_programs(0) - 1)
    def _():
        z_ref[...] = acc[...].astype(BF16)


def expert_forward(x, w_in, w_out, j, block, chunk):
    rows, d_model = x.shape
    d_ff = w_in.shape[2]
    return pl.pallas_call(
        functools.partial(forward_kernel, chunk),
        out_shape=jax.ShapeDtypeStruct((rows, d_model), BF16),
        grid=(d_ff // block,),
        in_specs=[
            pl.BlockSpec((rows, d_model), lambda f: (0, 0)),
            pl.BlockSpec((1, d_model, block), lambda f: (j, 0, f)),
            pl.BlockSpec((1, block, d_model), lambda f: (j, f, 0)),
        ],
        out_specs=pl.BlockSpec((rows, d_model), lambda f: (0, 0)),
        scratch_shapes=[VMEM((rows, d_model), F32)],
        compiler_params=pltpu.CompilerParams(vmem_limit_bytes=60 * 1024 * 1024),
        cost_estimate=pl.CostEstimate(flops=4 * rows * d_model * d_ff, bytes_accessed=16_000_000, transcendentals=rows * d_ff),
        name="expert_forward",
    )(x, w_in, w_out)


def backward_kernel(chunk, x_ref, dout_ref, z_ref, gate_ref, w1_ref, w2_ref, *refs):
    dx_ref, dw1_ref, dw2_ref, dg_ref, acc, dz, x_t, dz_t, h_buf, da_buf = refs[-10:]
    f = pl.program_id(0)
    rows = x_ref.shape[0]

    @pl.when(f == 0)
    def _():
        acc[...] = jnp.zeros_like(acc)

        def prepare(i, _):
            here = pl.ds(pl.multiple_of(i * 128, 128), 128)
            dout = dout_ref[here, :].astype(F32)
            prod = dout * z_ref[here, :].astype(F32)
            part = prod[:, 0:128]
            for c in range(128, prod.shape[1], 128):
                part = part + prod[:, c : c + 128]
            gate_row = gate_ref[pl.ds(i, 1), :]
            dg_ref[pl.ds(i, 1), :] = jnp.where(gate_row != 0.0, jnp.sum(part.T, axis=0, keepdims=True), 0.0)
            gate = jnp.broadcast_to(gate_row, (128, 128)).T
            for c in range(0, prod.shape[1], 128):
                dz[here, c : c + 128] = (gate * dout[:, c : c + 128]).astype(BF16)
            x_t[:, here] = x_ref[here, :].T
            dz_t[:, here] = dz[here, :].T
            return 0

        lax.fori_loop(0, rows // 128, prepare, 0)

    spans = [pl.ds(m, chunk) for m in range(0, rows, chunk)]
    ahead = dot_nn(x_ref[spans[0], :], w1_ref[0]), dot_nt(dz[spans[0], :], w2_ref[0])
    for i, here in enumerate(spans):
        a, back = ahead
        if i + 1 < len(spans):
            then = spans[i + 1]
            ahead = dot_nn(x_ref[then, :], w1_ref[0]), dot_nt(dz[then, :], w2_ref[0])
        sq = a * a
        t = jnp.tanh(a * (GELU_A + GELU_B * sq))
        q = 0.5 + 0.5 * t
        h_buf[here, :] = (a * q).astype(BF16)
        slope = q + (a * (GELU_A + (3.0 * GELU_B) * sq)) * (0.5 - 0.5 * (t * t))
        da = (slope * back).astype(BF16)
        da_buf[here, :] = da
        acc[here, :] += dot_nt(da, w1_ref[0])

    dw1_ref[0] = dot_nn(x_t[...], da_buf[...]).astype(BF16)
    dw2_ref[0] = dot_nn(dz_t[...], h_buf[...]).T.astype(BF16)

    @pl.when(f == pl.num_programs(0) - 1)
    def _():
        dx_ref[...] = acc[...].astype(BF16)


def expert_backward(x, dout, z, gate, w_in, w_out, grads, j, block, chunk):
    rows, d_model = x.shape
    d_ff = w_in.shape[2]
    one = pl.Buffered(1)
    whole = pl.BlockSpec((rows, d_model), lambda f: (0, 0), pipeline_mode=one)
    lines = pl.BlockSpec((rows // 128, 128), lambda f: (0, 0))
    return pl.pallas_call(
        functools.partial(backward_kernel, chunk),
        out_shape=(
            jax.ShapeDtypeStruct((rows, d_model), BF16),
            jax.ShapeDtypeStruct(w_in.shape, BF16),
            jax.ShapeDtypeStruct(w_out.shape, BF16),
            jax.ShapeDtypeStruct((rows // 128, 128), F32),
        ),
        grid=(d_ff // block,),
        in_specs=[
            whole,
            whole,
            whole,
            lines,
            pl.BlockSpec((1, d_model, block), lambda f: (j, 0, f)),
            pl.BlockSpec((1, block, d_model), lambda f: (j, f, 0)),
        ]
        + [pl.BlockSpec(memory_space=pl.ANY)] * len(grads),
        out_specs=(
            pl.BlockSpec((rows, d_model), lambda f: (0, 0), pipeline_mode=one),
            pl.BlockSpec((1, d_model, block), lambda f: (j, 0, f)),
            pl.BlockSpec((1, block, d_model), lambda f: (j, f, 0)),
            lines,
        ),
        scratch_shapes=[
            VMEM((rows, d_model), F32),
            VMEM((rows, d_model), BF16),
            VMEM((d_model, rows), BF16),
            VMEM((d_model, rows), BF16),
            VMEM((rows, block), BF16),
            VMEM((rows, block), BF16),
        ],
        compiler_params=pltpu.CompilerParams(vmem_limit_bytes=62 * 1024 * 1024),
        cost_estimate=pl.CostEstimate(flops=10 * rows * d_model * d_ff, bytes_accessed=32_000_000, transcendentals=rows * d_ff),
        input_output_aliases={6: 1, 7: 2} if grads else {},
        name="expert_backward",
    )(x, dout, z, gate.reshape(rows // 128, 128), w_in, w_out, *grads)


def solution(mesh):
    group = mesh.shape["ep"]
    token_spec = P(("dp", "ep"), None)
    weight_spec = P("ep", None, None)
    grad_spec = P(("dp", "ep"), None, None)

    def layer(hidden, logits, w_in, w_out, grad_out):
        tok_loc, _ = hidden.shape
        exp_count = logits.shape[1]
        exp_loc = w_in.shape[0]
        capacity = tok_loc * group * CAP_FACTOR // exp_count
        pair_cap = 2 * capacity // group
        rows = -(-(capacity + group * (ALIGN - 1)) // 128) * 128

        x_all = lax.all_gather(hidden, "ep", axis=0, tiled=True)
        dout_all = lax.all_gather(grad_out, "ep", axis=0, tiled=True)

        top = jnp.max(logits, axis=-1)
        den = jnp.sum(jnp.exp(logits - top[:, None]), axis=-1)
        gates = jnp.exp(logits - top[:, None]) / den[:, None]
        cand_val, cand_pos = lax.top_k(logits.T, pair_cap)
        sent = jnp.stack([cand_val, cand_pos.astype(F32)], axis=1)
        got = lax.all_to_all(sent, "ep", 0, 0, tiled=True).reshape(group, exp_loc, 2, pair_cap).transpose(1, 2, 0, 3)
        got_val = got[:, 0]
        merged = got_val.reshape(exp_loc, group * pair_cap)
        thresh_own = lax.top_k(merged, capacity)[0][:, capacity - 1]

        got_keep = got_val >= thresh_own[:, None, None]
        n_own = jnp.sum(got_keep.astype(jnp.int32), axis=-1)
        len_own = (n_own + ALIGN - 1) // ALIGN * ALIGN
        base_own = jnp.cumsum(len_own, axis=1) - len_own
        got_tok = got[:, 1].astype(jnp.int32) + (jnp.arange(group, dtype=jnp.int32) * tok_loc)[None, :, None]
        safe = jnp.max(jnp.where(got_keep[:, :, 0], got_tok[:, :, 0], -1), axis=1)
        got_tok = jnp.where(got_keep, got_tok, safe[:, None, None])
        tok_own = compact(got_tok, len_own, base_own, safe, rows)

        thresh_own, tok_own = lax.optimization_barrier((thresh_own, tok_own))
        facts = lax.all_gather(jnp.concatenate([thresh_own[:, None], base_own.astype(F32)], axis=1), "ep", tiled=True)
        keep = cand_val >= facts[:, :1]
        off_loc = lax.dynamic_index_in_dim(facts, lax.axis_index("ep") + 1, axis=1, keepdims=False).astype(jnp.int32)
        n_loc = jnp.sum(keep.astype(jnp.int32), axis=1)
        len_loc = (n_loc + ALIGN - 1) // ALIGN * ALIGN
        top_sel, den_sel = candidate_stats(cand_pos, len_loc, top, den)
        gate_sel = jnp.where(keep, jnp.exp(cand_val - top_sel) / den_sel, 0.0)
        got_gate = lax.all_to_all(gate_sel, "ep", 0, 0, tiled=True).reshape(group, exp_loc, pair_cap).transpose(1, 0, 2)
        gate_own = compact(got_gate, len_own, base_own, jnp.zeros((exp_loc,), F32), rows)

        perm = jnp.bitwise_xor(lax.axis_index("ep"), jnp.arange(group))
        ids = (perm[None, :] * exp_loc + jnp.arange(exp_loc)[:, None]).astype(jnp.int32)
        base_by, len_by = base_own[:, perm], len_own[:, perm]

        def go_back(rows_by):
            back = [rows_by[0]]
            for p in range(1, group):
                back.append(lax.ppermute(rows_by[p], "ep", [(i, i ^ p) for i in range(group)]))
            return back

        tok_own, gate_own = lax.optimization_barrier((tok_own, gate_own))

        block, chunk = 512, rows // 4
        saved = []
        for j in range(exp_loc):
            x = x_all.at[tok_own[j]].get(mode="promise_in_bounds")
            z = expert_forward(x, w_in, w_out, j, block, chunk)
            saved.append((x, z))
        ready, dout_all = lax.optimization_barrier((spread_all([z for _, z in saved], base_own, len_own, pair_cap), dout_all))
        z_back = lax.all_to_all(ready, "ep", 0, 0, tiled=True)

        grads, dx_back, dgates = (), [], []
        for j in range(exp_loc):
            x, z = saved[j]
            dout = dout_all.at[tok_own[j]].get(mode="promise_in_bounds")
            dx, *grads, dgate = expert_backward(x, dout, z, gate_own[j], w_in, w_out, grads, j, block, chunk)
            ready = spread(dx, base_by[j], len_by[j], pair_cap)
            dx_back += go_back(ready)
            dgates.append(dgate.reshape(rows))

        dg_own = jnp.stack(dgates)
        dg_all = lax.all_to_all(jnp.broadcast_to(dg_own[None], (group, exp_loc, rows)), "ep", 0, 0, tiled=True)
        off = off_loc + jnp.arange(exp_count, dtype=jnp.int32) * rows
        order = ids.reshape(-1)
        lens, poss = len_loc[order], cand_pos[order]
        (layer_out,) = combine(hidden, [z_back], len_loc, cand_pos, BF16, gate=gate_sel)
        cut = group * (exp_loc - 1) + 1
        part, dg_wide = combine(grad_out, dx_back[:cut], lens, poss, F32, marks=[order, off[order], dg_all.reshape(-1)])
        (grad_hidden,) = combine(part, dx_back[cut:], lens[cut:], poss[cut:], BF16)
        dgate = dg_wide[:, :exp_count]
        grad_logits = gates * (dgate - jnp.sum(gates * dgate, axis=-1, keepdims=True))
        return layer_out, grad_hidden, grad_logits, *grads

    return jax.shard_map(layer, mesh=mesh, in_specs=(token_spec, token_spec, weight_spec, weight_spec, token_spec), out_specs=(token_spec, token_spec, token_spec, grad_spec, grad_spec), check_vma=False)
```
